32 devices in a mesh: owner: 16 (over z, x, core), rep: 2 (over y).
Axes of the slice: x: 2, y: 2, z: 4, core: 2. Of those that a mesh axis runs over, the one named last changes fastest.
Arguments:
- features: float32 [16384, 256], P(('owner', 'rep')), may hold values from -6 to 6
- group_ids: int32 [16384], P(('owner', 'rep')), may hold values from 0 to 65535, as said below
- survive: int32 [16384], P(('owner', 'rep')), may hold values from 0 to 1
- home_row: int32 [65536], replicated, may hold values from 0 to 65535, as said below
- hot_ids: int32 [256], replicated, may hold values from 0 to 65535, as said below
Outputs:
- group_out: float32 [65536, 256], P(('owner', 'rep'))
- group_count: float32 [65536], P(('owner', 'rep'))
- hot_out: float32 [256, 256], P('rep')
- hot_count: float32 [256], P('rep')
The draws below stay inside these ranges and needn't reach their ends.
Inputs may be any that keep to these rules, and one draw needn't show every extreme that they name: home_row is a permutation of the groups. hot_ids holds 256 different groups. `group_ids`: among the rows of one device, 128 name hot groups, and at most 64 rows name non-hot groups g whose home_row[g] // 4096 is one and the same owner index; on every device some owners get exactly 64 such rows.
All inputs are finite; a program needn't handle non-finite values.
Results may differ from the reference program's by a relative error of at most 0.00007.
Values sent between devices are 32-bit elements; how exact they have to be, the bound alone decides.
A program may use at most 64 MiB of HBM per device.

```python
import jax
import jax.numpy as jnp

F = 256
GROUPS = 65536
HOT = 256
ROWS_DEV = 512
ROWS = 16384
OWN_GROUPS = 4096
CAP = 64
HOT_ROWS = 128
N_OWNER = 16
DEVICES = 32


def shared_tables(key):
    home = jax.random.permutation(jax.random.fold_in(key, 11), GROUPS).astype(jnp.int32)
    inverse = jnp.zeros((GROUPS,), jnp.int32).at[home].set(jnp.arange(GROUPS, dtype=jnp.int32))
    index = jnp.arange(HOT, dtype=jnp.int32)
    hot = inverse[index % N_OWNER * OWN_GROUPS + OWN_GROUPS - 1 - index // N_OWNER]
    return (home, inverse, hot)


def draw_home_row(key, part):
    return shared_tables(key)[0]


def draw_hot_ids(key, part):
    return shared_tables(key)[2]


def row_layout(key):
    home, inverse, hot = shared_tables(key)
    cold_rows = ROWS_DEV - HOT_ROWS
    span = OWN_GROUPS - HOT // N_OWNER
    chosen = jax.random.randint(jax.random.fold_in(key, 31), (), 0, N_OWNER).astype(jnp.int32)

    def one_device(dev_key):
        keys = jax.random.split(dev_key, 6)
        limit = jax.random.randint(keys[0], (HOT_ROWS,), 1, HOT + 1)
        pick = jax.random.randint(keys[1], (HOT_ROWS,), 0, 1 << 20) % limit
        hot_part = hot[pick]
        shuffled = jax.random.permutation(keys[2], N_OWNER).astype(jnp.int32)
        where_chosen = jnp.argmax((shuffled == chosen).astype(jnp.int32)).astype(jnp.int32)
        first = shuffled[0]
        owners = shuffled.at[where_chosen].set(first).at[0].set(chosen)
        owner = owners[jnp.arange(cold_rows, dtype=jnp.int32) // CAP]
        limit_cold = jax.random.randint(keys[3], (cold_rows,), 1, span + 1)
        within = jax.random.randint(keys[4], (cold_rows,), 0, 1 << 20) % limit_cold
        cold_part = inverse[owner * OWN_GROUPS + within]
        ids = jnp.concatenate([hot_part, cold_part]).astype(jnp.int32)
        flagged = jnp.concatenate([jnp.zeros((HOT_ROWS,), jnp.int32), (owner == chosen).astype(jnp.int32)])
        order = jax.random.permutation(keys[5], ROWS_DEV)
        return (ids[order], flagged[order])
    dev_keys = jax.random.split(jax.random.fold_in(key, 23), DEVICES)
    ids, flagged = jax.vmap(one_device)(dev_keys)
    return (ids.astype(jnp.int32), flagged.astype(jnp.int32))


def draw_group_ids(key, part):
    return row_layout(key)[0].reshape(-1).astype(jnp.int32)


def draw_survive(key, part):
    flagged = row_layout(key)[1]
    coin = jax.random.randint(jax.random.fold_in(key, 41), (DEVICES, ROWS_DEV), 0, 2).astype(jnp.int32)
    full_device = jax.random.randint(jax.random.fold_in(key, 43), (DEVICES,), 0, 16) == 0
    alive = jnp.where((flagged == 1) | full_device[:, None], 1, coin)
    return alive.reshape(-1).astype(jnp.int32)


def level_of(own_key, extent, cuts, low, largest):
    def one(axis_at, parts):
        heights = jax.random.uniform(jax.random.fold_in(jax.random.fold_in(own_key, 6), axis_at), (parts,), jnp.float32, low / len(cuts), largest / len(cuts))
        return jnp.repeat(jnp.exp(heights), extent[axis_at] // parts).reshape((-1,) + (1,) * (len(extent) - axis_at - 1))

    level = one(*cuts[0])
    for cut in cuts[1:]:
        level = level * one(*cut)
    return level


def bell_draw(rng, shape, deviation, most, cuts=(), kind=jnp.bfloat16):
    factor_of = level_of(rng, shape, cuts, -0.22, 0.18) if cuts else 1.0
    drawn = jax.random.normal(rng, shape, jnp.float32) * deviation * factor_of
    return jnp.minimum(jnp.maximum(drawn, -most), most).astype(kind)


def setup_inputs(seed: int = 0) -> dict:
    arg_keys = jax.random.split(jax.random.key(seed), 6)
    features = bell_draw(arg_keys[0], (ROWS, F), 1.0, 6.0, ((0, 32),), jnp.float32)
    group_ids = draw_group_ids(jax.random.fold_in(arg_keys[5], 71), 0)
    survive = draw_survive(jax.random.fold_in(arg_keys[5], 71), 0)
    home_row = draw_home_row(jax.random.fold_in(arg_keys[5], 71), 0)
    hot_ids = draw_hot_ids(jax.random.fold_in(arg_keys[5], 71), 0)
    return {"features": features, "group_ids": group_ids, "survive": survive, "home_row": home_row, "hot_ids": hot_ids}


def reference(features, group_ids, survive, home_row, hot_ids):
    weight = jnp.where(survive == 1, 1.0, 0.0).astype(jnp.float32)
    hot_slot = jnp.zeros((GROUPS,), jnp.int32).at[hot_ids].set(jnp.arange(1, HOT + 1, dtype=jnp.int32))
    hot_of_row = hot_slot[group_ids]
    kept = features * weight[:, None]
    cold_target = jnp.where(hot_of_row > 0, GROUPS, home_row[group_ids]).astype(jnp.int32)
    hot_target = jnp.where(hot_of_row > 0, hot_of_row - 1, HOT).astype(jnp.int32)
    cold_sum = jax.ops.segment_sum(kept, cold_target, num_segments=GROUPS + 1)[:GROUPS]
    cold_count = jax.ops.segment_sum(weight, cold_target, num_segments=GROUPS + 1)[:GROUPS]
    hot_sum = jax.ops.segment_sum(kept, hot_target, num_segments=HOT + 1)[:HOT]
    hot_count = jax.ops.segment_sum(weight, hot_target, num_segments=HOT + 1)[:HOT]
    group_out = cold_sum / jnp.sqrt(1.0 + cold_count)[:, None]
    hot_out = hot_sum / jnp.sqrt(1.0 + hot_count)[:, None]
    return (group_out, cold_count, hot_out, hot_count)
```

```python
import functools

import jax
import jax.numpy as jnp
from jax import lax
from jax.experimental import pallas as pl
from jax.experimental.pallas import tpu as pltpu
from jax.sharding import PartitionSpec as P

MESH = pl.DeviceIdType.MESH
LANES = 128
SUB = 8
BF = jnp.bfloat16
F32 = jnp.float32


def iota(shape, axis):
    return lax.broadcasted_iota(jnp.int32, shape, axis)


def mm(a, b, dims=((1,), (0,))):
    return lax.dot_general(a, b, (dims, ((), ())), preferred_element_type=F32)


def split(x):
    hi = x.astype(BF)
    return hi, (x - hi.astype(F32)).astype(BF)


def kernel(
    cfg,
    ids_ref,
    survive_ref,
    hot_ref,
    table_ref,
    feat_ref,
    sum_ref,
    count_ref,
    hot_sum_ref,
    hot_count_ref,
    bucket,
    arrived,
    hot_part,
    hot_in,
    hot_red,
    hot_all,
    send1,
    recv1,
    send2,
    recv2,
    hsend,
    hrecv,
    gsend,
    grecv,
):
    owners, reps, cap, own_groups, home_dev = cfg
    rows, width = feat_ref.shape
    hots = hot_ref.shape[1]
    nb = width // cap
    chunks = owners // nb
    pieces = hots // reps // SUB
    ndev = owners * reps
    me = lax.axis_index("owner")
    rep = lax.axis_index("rep")
    dev = me * reps + rep

    barrier = pltpu.get_barrier_semaphore()

    @pl.loop(1, ndev)
    def _(d):
        other = lax.rem(dev + d, ndev)
        pl.semaphore_signal(
            barrier, inc=1, device_id=(other // reps, lax.rem(other, reps)), device_id_type=MESH
        )

    ids = ids_ref[...]
    live = survive_ref[...] == 1
    table = table_ref[...]
    trows = table.shape[0]
    halves = jnp.concatenate([table >> 8, table & 255], axis=1).astype(F32).astype(BF)
    pick = jnp.where(iota((trows, rows), 0) == (ids >> 7), 1.0, 0.0).astype(BF)
    both = mm(halves, pick, ((0,), (0,)))
    column = both[:LANES] * 256.0 + both[LANES:]
    home = jnp.sum(
        jnp.where(iota((LANES, rows), 0) == (ids & (LANES - 1)), column, 0.0), axis=0, keepdims=True
    )
    target = jnp.floor(home * (1.0 / own_groups))
    label = home - target * own_groups + 1.0
    ahead = target - me.astype(F32)
    ahead = jnp.where(ahead < 0.0, ahead + owners, ahead)

    hot_col = jnp.sum(
        jnp.where(iota((hots, hots), 0) == iota((hots, hots), 1), hot_ref[...].astype(F32), 0.0),
        axis=1,
        keepdims=True,
    )
    matches = jnp.where(hot_col == ids.astype(F32), 1.0, 0.0)
    is_hot = jnp.max(matches, axis=0, keepdims=True)
    live_f = jnp.where(live, 1.0, 0.0)
    keep = live_f * (1.0 - is_hot)
    ahead = jnp.where(keep > 0.0, ahead, -1.0)
    ahead_i = ahead.astype(jnp.int32)

    member = jnp.where(iota((owners, rows), 0) == ahead_i, 1.0, 0.0)
    before = jnp.where(iota((rows, rows), 0) < iota((rows, rows), 1), 1.0, 0.0).astype(BF)
    position = mm(member.astype(BF), before)
    placed = jnp.sum(position * member, axis=0, keepdims=True)
    slot = jnp.where(keep > 0.0, ahead * cap + placed, -1.0).astype(jnp.int32)
    lane = (placed + cap * (ahead - nb * jnp.floor(ahead * (1.0 / nb)))).astype(jnp.int32)
    label_hi = jnp.floor(label * (1.0 / 256.0))
    label_lo = label - 256.0 * label_hi
    coded = jnp.concatenate([member * label_hi, member * label_lo], axis=0).astype(BF)
    where = jnp.where(iota((width, rows), 0) == lane, 1.0, 0.0).astype(BF)
    coded = mm(coded, where, ((1,), (1,)))
    labels = coded[:owners] * 256.0 + coded[owners:]

    feat_hi, feat_lo = split(feat_ref[...])
    blocks = []
    for c in range(chunks):
        place = jnp.where(iota((width, rows), 0) + c * width == slot, 1.0, 0.0).astype(BF)
        packed = mm(place, feat_hi) + mm(place, feat_lo)
        for i in range(nb):
            k = c * nb + i
            dst = arrived.at[0, 0] if k == 0 else bucket.at[k - 1]
            dst[:cap, :] = packed[i * cap : (i + 1) * cap]
            dst[cap:, :] = jnp.broadcast_to(labels[k : k + 1], (SUB, width))

    pl.semaphore_wait(barrier, ndev - 1)

    def send_block(k):
        return pltpu.make_async_remote_copy(
            src_ref=bucket.at[k - 1],
            dst_ref=arrived.at[0, k],
            send_sem=send1,
            recv_sem=recv1.at[k],
            device_id=(lax.rem(me + k, owners), rep),
            device_id_type=MESH,
        )

    def forward(q, k):
        return pltpu.make_async_remote_copy(
            src_ref=arrived.at[0, k],
            dst_ref=arrived.at[q, k],
            send_sem=send2,
            recv_sem=recv2.at[q, k],
            device_id=(me, lax.rem(rep + q, reps)),
            device_id_type=MESH,
        )

    def forward_all(k):
        for q in range(1, reps):
            forward(q, k).start()

    @pl.loop(1, owners)
    def _(k):
        send_block(k).start()

    forward_all(0)

    hot_table = matches * live_f
    tally = jnp.sum(hot_table, axis=1, keepdims=True)
    hot_bf = hot_table.astype(BF)
    sums = mm(hot_bf, feat_hi) + mm(hot_bf, feat_lo)
    hot_part[:, :, :width] = sums.reshape(hots // SUB, SUB, width)
    hot_part[:, :, width:] = jnp.broadcast_to(tally, (hots, LANES)).reshape(hots // SUB, SUB, LANES)

    def hot_send(b):
        to_owner = lax.rem(b, pieces)
        to_rep = b // pieces
        to = to_owner * reps + to_rep
        back = lax.rem(to - dev + ndev, ndev)
        return to, pltpu.make_async_remote_copy(
            src_ref=hot_part.at[b],
            dst_ref=hot_in.at[back],
            send_sem=hsend.at[b],
            recv_sem=hrecv,
            device_id=(to_owner, to_rep),
            device_id_type=MESH,
        )

    @pl.loop(0, hots // SUB)
    def _(b):
        to, copy = hot_send(b)

        @pl.when(to != dev)
        def _():
            copy.start()

    tiles = max(1, home_dev // 512)
    tile = home_dev // tiles
    base = rep * home_dev + 1
    sum_ref[...] = jnp.zeros_like(sum_ref)
    count_ref[...] = jnp.zeros_like(count_ref)

    def add_chunk(q, c):
        lab = arrived[q, c * nb, cap : cap + SUB, :]
        for i in range(1, nb):
            lab = lab + arrived[q, c * nb + i, cap : cap + SUB, :]
        lab = lab[:1].astype(jnp.int32) - base
        block = jnp.concatenate([arrived[q, c * nb + i, :cap, :] for i in range(nb)], axis=0)
        hi, lo = split(block)
        ones = jnp.ones((SUB, width), BF)

        for t in range(tiles):
            onehot = jnp.where(iota((tile, width), 0) + t * tile == lab, 1.0, 0.0).astype(BF)
            at = pl.ds(t * tile, tile)
            sum_ref[at, :] += mm(onehot, hi) + mm(onehot, lo)
            count_ref[:, at] += mm(ones, onehot, ((1,), (1,)))

    def own_chunk(c):
        @pl.loop(max(1, c * nb), (c + 1) * nb)
        def _(k):
            send_block(k).wait_recv()
            forward_all(k)

        add_chunk(0, c)

    def peer_chunk(c):
        for q in range(1, reps):

            @pl.loop(c * nb, (c + 1) * nb)
            def _(k):
                forward(q, k).wait_recv()

            add_chunk(q, c)

    def hot_gather(d):
        return pltpu.make_async_remote_copy(
            src_ref=hot_red,
            dst_ref=hot_all.at[me],
            send_sem=gsend.at[d],
            recv_sem=grecv.at[me],
            device_id=(lax.rem(me + d, owners), rep),
            device_id_type=MESH,
        )

    own_chunk(0)

    @pl.when(me < pieces)
    def _():
        mine = hot_in.at[pl.ds(1, ndev - 1)]
        pltpu.make_async_copy(mine, mine, hrecv).wait()
        total = hot_part[rep * pieces + me] + jnp.sum(hot_in[1:], axis=0)
        hot_red[...] = total
        hot_all[me] = total

        @pl.loop(1, owners)
        def _(d):
            hot_gather(d).start()

    for c in range(1, chunks):
        own_chunk(c)
        peer_chunk(c - 1)
    peer_chunk(chunks - 1)

    @pl.loop(0, pieces)
    def _(p):
        @pl.when(p != me)
        def _():
            pltpu.make_async_copy(hot_all.at[p], hot_all.at[p], grecv.at[p]).wait()

    per_rep = pieces * SUB
    everything = hot_all[...].reshape(per_rep, width + LANES)
    hot_sum_ref[...] = everything[:, :width]
    counts = everything[:, width:]
    diagonal = jnp.where(iota((per_rep, LANES), 0) == iota((per_rep, LANES), 1), counts, 0.0)
    hot_count_ref[...] = jnp.broadcast_to(jnp.sum(diagonal, axis=0, keepdims=True), (SUB, LANES))

    @pl.when(me < pieces)
    def _():
        @pl.loop(1, owners)
        def _(d):
            hot_gather(d).wait_send()

    @pl.loop(0, hots // SUB)
    def _(b):
        to, copy = hot_send(b)

        @pl.when(to != dev)
        def _():
            copy.wait_send()

    pltpu.make_async_copy(bucket, bucket, send1).wait()
    if reps > 1:
        sent = arrived.at[pl.ds(1, reps - 1)]
        pltpu.make_async_copy(sent, sent, send2).wait()


def local(features, group_ids, survive, home_row, hot_ids):
    rows, width = features.shape
    owners = lax.axis_size("owner")
    reps = lax.axis_size("rep")
    groups = home_row.shape[0]
    hots = hot_ids.shape[0]
    own_groups = groups // owners
    home_dev = own_groups // reps
    cap = 2 * rows // owners
    pieces = hots // reps // SUB
    cfg = (owners, reps, cap, own_groups, home_dev)
    vmem = pl.BlockSpec(memory_space=pltpu.VMEM)
    DMA = pltpu.SemaphoreType.DMA
    cold_sum, count, hot_sum, hot_count = pl.pallas_call(
        functools.partial(kernel, cfg),
        out_shape=(
            jax.ShapeDtypeStruct((home_dev, width), F32),
            jax.ShapeDtypeStruct((SUB, home_dev), F32),
            jax.ShapeDtypeStruct((hots // reps, width), F32),
            jax.ShapeDtypeStruct((SUB, LANES), F32),
        ),
        in_specs=[vmem] * 5,
        out_specs=[vmem] * 4,
        scratch_shapes=[
            pltpu.VMEM((owners - 1, cap + SUB, width), F32),
            pltpu.VMEM((reps, owners, cap + SUB, width), F32),
            pltpu.VMEM((hots // SUB, SUB, width + LANES), F32),
            pltpu.VMEM((owners * reps, SUB, width + LANES), F32),
            pltpu.VMEM((SUB, width + LANES), F32),
            pltpu.VMEM((pieces, SUB, width + LANES), F32),
            DMA(()),
            DMA((owners,)),
            DMA(()),
            DMA((reps, owners)),
            DMA((hots // SUB,)),
            DMA(()),
            DMA((owners,)),
            DMA((pieces,)),
        ],
        compiler_params=pltpu.CompilerParams(
            collective_id=0, has_side_effects=True, vmem_limit_bytes=48 << 20
        ),
    )(
        group_ids.reshape(1, rows),
        survive.reshape(1, rows),
        hot_ids.reshape(1, hots),
        home_row.reshape(groups // LANES, LANES),
        features,
    )
    group_count = count[0]
    counts_hot = hot_count[0, : hots // reps]
    group_out = cold_sum / jnp.sqrt(1.0 + group_count)[:, None]
    hot_out = hot_sum / jnp.sqrt(1.0 + counts_hot)[:, None]
    return group_out, group_count, hot_out, counts_hot


def solution(mesh):
    in_specs = (P(("owner", "rep"), None), P(("owner", "rep")), P(("owner", "rep")), P(), P())
    out_specs = (P(("owner", "rep"), None), P(("owner", "rep")), P("rep", None), P("rep"))
    return jax.shard_map(local, mesh=mesh, in_specs=in_specs, out_specs=out_specs, check_vma=False)
```

```python
import functools

import jax
import jax.numpy as jnp
from jax import lax
from jax.experimental import pallas as pl
from jax.experimental.pallas import tpu as pltpu
from jax.sharding import PartitionSpec as P

MESH = pl.DeviceIdType.MESH
LANES = 128
SUB = 8
BF = jnp.bfloat16
F32 = jnp.float32


def iota(shape, axis):
    return lax.broadcasted_iota(jnp.int32, shape, axis)


def mm(a, b, dims=((1,), (0,))):
    return lax.dot_general(a, b, (dims, ((), ())), preferred_element_type=F32)


def split(x):
    hi = x.astype(BF)
    return hi, (x - hi.astype(F32)).astype(BF)


def kernel(
    cfg,
    ids_hbm,
    survive_hbm,
    hot_hbm,
    table_hbm,
    feat_hbm,
    sum_ref,
    count_ref,
    hot_sum_ref,
    hot_count_ref,
    ids_ref,
    survive_ref,
    hot_ref,
    table_ref,
    feat_ref,
    bucket,
    arrived,
    tags,
    tags_in,
    hot_part,
    hot_l1,
    hot_s1,
    hot_l2,
    hot_s2,
    hot_l3,
    hot_red,
    hot_all,
    load,
    send1,
    recv1,
    send2,
    recv2,
    tsend,
    trecv,
    s_core,
    r_core,
    s_rep,
    r_rep,
    s_chip,
    r_chip,
    s_all,
    r_all,
    s_last,
    r_last,
):
    owners, reps, cap, own_groups, home_dev = cfg
    rows, width = feat_ref.shape
    hots = hot_ref.shape[1]
    nb = width // cap
    chunks = owners // nb
    chips = owners // 2
    pieces = hots // reps // 2 // SUB
    part = pieces * SUB
    ndev = owners * reps
    half = owners // 2
    quarter = owners // 4
    me = lax.axis_index("owner")
    rep = lax.axis_index("rep")
    dev = me * reps + rep
    core = lax.rem(me, 2)
    chip = me // 2

    loads = [
        pltpu.make_async_copy(src, dst, load.at[i])
        for i, (src, dst) in enumerate(
            (
                (table_hbm, table_ref),
                (ids_hbm, ids_ref),
                (survive_hbm, survive_ref),
                (hot_hbm, hot_ref),
                (feat_hbm, feat_ref),
            )
        )
    ]
    for copy in loads:
        copy.start()

    barrier = pltpu.get_barrier_semaphore()

    @pl.loop(1, ndev)
    def _(d):
        other = lax.rem(dev + d, ndev)
        pl.semaphore_signal(
            barrier, inc=1, device_id=(other // reps, lax.rem(other, reps)), device_id_type=MESH
        )

    flips = []
    bit = 1
    while bit < owners:
        flips.append((bit, bit - 2 * bit * lax.rem(me // bit, 2)))
        bit *= 2

    def partner(p):
        v = p - half
        number = p if p < half else half + v // 2 + (v % 2) * quarter
        out = me
        for bit, flip in flips:
            if number & bit:
                out = out + flip
        return out

    for copy in loads[:4]:
        copy.wait()
    ids = ids_ref[...]
    live_f = jnp.where(survive_ref[...] == 1, 1.0, 0.0)
    table = table_ref[...]
    trows = table.shape[0]
    halves = jnp.concatenate([table >> 8, table & 255], axis=1).astype(F32).astype(BF)
    pick = jnp.where(iota((trows, rows), 0) == (ids >> 7), 1.0, 0.0).astype(BF)
    both = mm(halves, pick, ((0,), (0,)))
    column = both[:LANES] * 256.0 + both[LANES:]
    home = jnp.sum(
        jnp.where(iota((LANES, rows), 0) == (ids & (LANES - 1)), column, 0.0), axis=0, keepdims=True
    )
    target = jnp.floor(home * (1.0 / own_groups))
    label = home - target * own_groups + 1.0
    number = target.astype(jnp.int32) ^ me
    low = number & (half - 1)
    spread = half + 2 * (low & (quarter - 1)) + jnp.where(low >= quarter, 1, 0)
    place_at = jnp.where(number < half, number, spread)

    hot_col = jnp.sum(
        jnp.where(iota((hots, hots), 0) == iota((hots, hots), 1), hot_ref[...].astype(F32), 0.0),
        axis=1,
        keepdims=True,
    )
    matches = jnp.where(hot_col == ids.astype(F32), 1.0, 0.0)
    is_hot = jnp.max(matches, axis=0, keepdims=True)
    keep = live_f * (1.0 - is_hot)
    place_at = jnp.where(keep > 0.0, place_at, -1)

    member = jnp.where(iota((owners, rows), 0) == place_at, 1.0, 0.0)
    before = jnp.where(iota((rows, rows), 0) < iota((rows, rows), 1), 1.0, 0.0).astype(BF)
    position = mm(member.astype(BF), before)
    placed = jnp.sum(position * member, axis=0, keepdims=True).astype(jnp.int32)
    slot = jnp.where(keep > 0.0, place_at * cap + placed, -1)
    lane = placed + cap * (place_at & (nb - 1))
    label_hi = jnp.floor(label * (1.0 / 256.0))
    label_lo = label - 256.0 * label_hi
    coded = jnp.concatenate([member * label_hi, member * label_lo], axis=0).astype(BF)
    where = jnp.where(iota((width, rows), 0) == lane, 1.0, 0.0).astype(BF)
    coded = mm(coded, where, ((1,), (1,)))
    labels = coded[:owners] * 256.0 + coded[owners:]
    for p in range(owners):
        tags[p] = labels[p : p + 1]

    def send_block(p):
        return pltpu.make_async_remote_copy(
            src_ref=bucket.at[p - 1],
            dst_ref=arrived.at[0, p],
            send_sem=send1,
            recv_sem=recv1.at[p],
            device_id=(partner(p), rep),
            device_id_type=MESH,
        )

    def send_tag(q, p):
        return pltpu.make_async_remote_copy(
            src_ref=tags.at[p],
            dst_ref=tags_in.at[q, p],
            send_sem=tsend.at[q, p],
            recv_sem=trecv.at[q, p],
            device_id=(partner(p), lax.rem(rep + q, reps)),
            device_id_type=MESH,
        )

    def forward(q, p):
        return pltpu.make_async_remote_copy(
            src_ref=arrived.at[0, p],
            dst_ref=arrived.at[q, p],
            send_sem=send2,
            recv_sem=recv2.at[q, p],
            device_id=(me, lax.rem(rep + q, reps)),
            device_id_type=MESH,
        )

    pairs = [(q, p) for p in range(owners) for q in range(reps) if q + p]
    tags_in[0, 0] = labels[:1]
    loads[4].wait()
    feat_hi, feat_lo = split(feat_ref[...])
    for c in range(chunks):
        place = jnp.where(iota((width, rows), 0) + c * width == slot, 1.0, 0.0).astype(BF)
        packed = mm(place, feat_hi) + mm(place, feat_lo)
        for i in range(nb):
            p = c * nb + i
            dst = arrived.at[0, 0] if p == 0 else bucket.at[p - 1]
            dst[...] = packed[i * cap : (i + 1) * cap]
        if c == 0:
            pl.semaphore_wait(barrier, ndev - 1)
        for p in range(c * nb, (c + 1) * nb):
            if p == 0:
                for q in range(1, reps):
                    forward(q, 0).start()
            else:
                send_block(p).start()
    for q, p in pairs:
        send_tag(q, p).start()

    hot_table = matches * live_f
    tally = jnp.sum(hot_table, axis=1, keepdims=True)
    hot_bf = hot_table.astype(BF)
    sums = mm(hot_bf, feat_hi) + mm(hot_bf, feat_lo)
    hot_part[:, :, :, :width] = sums.reshape(reps, 2, part, width)
    hot_part[:, :, :, width:] = jnp.broadcast_to(tally, (hots, LANES)).reshape(reps, 2, part, LANES)
    mate = (me + 1 - 2 * core, rep)
    to_core = pltpu.make_async_remote_copy(
        src_ref=hot_part.at[:, 1 - core],
        dst_ref=hot_l1,
        send_sem=s_core,
        recv_sem=r_core,
        device_id=mate,
        device_id_type=MESH,
    )
    to_core.start()

    def to_rep(q):
        other = lax.rem(rep + q, reps)
        return pltpu.make_async_remote_copy(
            src_ref=hot_s1.at[other],
            dst_ref=hot_l2.at[q],
            send_sem=s_rep.at[q],
            recv_sem=r_rep.at[q],
            device_id=(me, other),
            device_id_type=MESH,
        )

    def to_chip(p):
        return pltpu.make_async_remote_copy(
            src_ref=hot_s2.at[p],
            dst_ref=hot_l3.at[lax.rem(p - chip + chips, chips)],
            send_sem=s_chip.at[p],
            recv_sem=r_chip,
            device_id=(p * 2 + core, rep),
            device_id_type=MESH,
        )

    def to_all(d):
        return pltpu.make_async_remote_copy(
            src_ref=hot_red,
            dst_ref=hot_all.at[core, chip],
            send_sem=s_all.at[d],
            recv_sem=r_all.at[chip],
            device_id=(lax.rem(chip + d, chips) * 2 + core, rep),
            device_id_type=MESH,
        )

    to_mate = pltpu.make_async_remote_copy(
        src_ref=hot_all.at[core],
        dst_ref=hot_all.at[core],
        send_sem=s_last,
        recv_sem=r_last,
        device_id=mate,
        device_id_type=MESH,
    )

    def hot_step_1():
        to_core.wait_recv()
        hot_s1[...] = hot_part[:, core] + hot_l1[...]
        for q in range(1, reps):
            to_rep(q).start()

    def hot_step_2():
        total = hot_s1[rep]
        for q in range(1, reps):
            to_rep(q).wait_recv()
            total = total + hot_l2[q]
        hot_s2[...] = total.reshape(pieces, SUB, width + LANES)

        @pl.loop(0, pieces)
        def _(p):
            @pl.when(p != chip)
            def _():
                to_chip(p).start()

    def hot_step_3():
        @pl.when(chip < pieces)
        def _():
            mine = hot_l3.at[pl.ds(1, chips - 1)]
            pltpu.make_async_copy(mine, mine, r_chip).wait()
            total = hot_s2[chip] + jnp.sum(hot_l3[1:], axis=0)
            hot_red[...] = total
            hot_all[core, chip] = total

            @pl.loop(1, chips)
            def _(d):
                to_all(d).start()

    def hot_step_4():
        @pl.loop(0, pieces)
        def _(p):
            @pl.when(p != chip)
            def _():
                pltpu.make_async_copy(hot_all.at[core, p], hot_all.at[core, p], r_all.at[p]).wait()

        to_mate.start()

    def hot_step_5():
        to_mate.wait_recv()
        everything = hot_all[...].reshape(2 * part, width + LANES)
        hot_sum_ref[...] = everything[:, :width]
        counts = everything[:, width:]
        diagonal = jnp.where(iota((2 * part, LANES), 0) == iota((2 * part, LANES), 1), counts, 0.0)
        hot_count_ref[...] = jnp.broadcast_to(jnp.sum(diagonal, axis=0, keepdims=True), (SUB, LANES))

    tiles = max(1, home_dev // 512)
    tile = home_dev // tiles
    base = rep * home_dev + 1

    def add_chunk(q, c):
        first = q == 0 and c == 0
        lab = jnp.zeros((1, width), F32)
        for p in range(c * nb, (c + 1) * nb):
            if q + p:
                send_tag(q, p).wait_recv()
            lab = lab + tags_in[q, p]
        lab = lab.astype(jnp.int32) - base
        block = jnp.concatenate([arrived[q, c * nb + i] for i in range(nb)], axis=0)
        hi, lo = split(block)
        ones = jnp.ones((SUB, width), BF)

        for t in range(tiles):
            onehot = jnp.where(iota((tile, width), 0) + t * tile == lab, 1.0, 0.0).astype(BF)
            at = pl.ds(t * tile, tile)
            total = mm(onehot, hi) + mm(onehot, lo)
            tally = mm(ones, onehot, ((1,), (1,)))
            if first:
                sum_ref[at, :] = total
                count_ref[:, at] = tally
            else:
                sum_ref[at, :] += total
                count_ref[:, at] += tally

    def pass_on(c):
        for p in range(max(1, c * nb), (c + 1) * nb):
            send_block(p).wait_recv()
            for q in range(1, reps):
                forward(q, p).start()

    def peer_chunk(c):
        for q in range(1, reps):
            for p in range(c * nb, (c + 1) * nb):
                forward(q, p).wait_recv()
            add_chunk(q, c)

    steps = [hot_step_1, hot_step_2, hot_step_3]
    for c in range(chunks):
        pass_on(c)
        if steps:
            steps.pop(0)()
        add_chunk(0, c)
        if c:
            peer_chunk(c - 1)
    for step in steps:
        step()
    hot_step_4()
    hot_step_5()
    peer_chunk(chunks - 1)

    to_core.wait_send()
    for q in range(1, reps):
        to_rep(q).wait_send()

    @pl.loop(0, pieces)
    def _(p):
        @pl.when(p != chip)
        def _():
            to_chip(p).wait_send()

    @pl.when(chip < pieces)
    def _():
        @pl.loop(1, chips)
        def _(d):
            to_all(d).wait_send()

    to_mate.wait_send()
    for q, p in pairs:
        send_tag(q, p).wait_send()
    pltpu.make_async_copy(bucket, bucket, send1).wait()
    if reps > 1:
        sent = arrived.at[pl.ds(1, reps - 1)]
        pltpu.make_async_copy(sent, sent, send2).wait()


def local(features, group_ids, survive, home_row, hot_ids):
    rows, width = features.shape
    owners = lax.axis_size("owner")
    reps = lax.axis_size("rep")
    groups = home_row.shape[0]
    hots = hot_ids.shape[0]
    own_groups = groups // owners
    home_dev = own_groups // reps
    cap = 2 * rows // owners
    chips = owners // 2
    pieces = hots // reps // 2 // SUB
    part = pieces * SUB
    wide = width + LANES
    cfg = (owners, reps, cap, own_groups, home_dev)
    vmem = pl.BlockSpec(memory_space=pltpu.VMEM)
    hbm = pl.BlockSpec(memory_space=pltpu.HBM)
    DMA = pltpu.SemaphoreType.DMA
    VM = pltpu.VMEM
    cold_sum, count, hot_sum, hot_count = pl.pallas_call(
        functools.partial(kernel, cfg),
        out_shape=(
            jax.ShapeDtypeStruct((home_dev, width), F32),
            jax.ShapeDtypeStruct((SUB, home_dev), F32),
            jax.ShapeDtypeStruct((hots // reps, width), F32),
            jax.ShapeDtypeStruct((SUB, LANES), F32),
        ),
        in_specs=[hbm] * 5,
        out_specs=[vmem] * 4,
        scratch_shapes=[
            VM((1, rows), jnp.int32),
            VM((1, rows), jnp.int32),
            VM((1, hots), jnp.int32),
            VM((groups // LANES, LANES), jnp.int32),
            VM((rows, width), F32),
            VM((owners - 1, cap, width), F32),
            VM((reps, owners, cap, width), F32),
            VM((owners, 1, width), F32),
            VM((reps, owners, 1, width), F32),
            VM((reps, 2, part, wide), F32),
            VM((reps, part, wide), F32),
            VM((reps, part, wide), F32),
            VM((reps, part, wide), F32),
            VM((pieces, SUB, wide), F32),
            VM((chips, SUB, wide), F32),
            VM((SUB, wide), F32),
            VM((2, pieces, SUB, wide), F32),
            DMA((5,)),
            DMA(()),
            DMA((owners,)),
            DMA(()),
            DMA((reps, owners)),
            DMA((reps, owners)),
            DMA((reps, owners)),
            DMA(()),
            DMA(()),
            DMA((reps,)),
            DMA((reps,)),
            DMA((pieces,)),
            DMA(()),
            DMA((chips,)),
            DMA((pieces,)),
            DMA(()),
            DMA(()),
        ],
        compiler_params=pltpu.CompilerParams(
            collective_id=0, has_side_effects=True, vmem_limit_bytes=48 << 20
        ),
    )(
        group_ids.reshape(1, rows),
        survive.reshape(1, rows),
        hot_ids.reshape(1, hots),
        home_row.reshape(groups // LANES, LANES),
        features,
    )
    group_count = count[0]
    counts_hot = hot_count[0, : hots // reps]
    group_out = cold_sum / jnp.sqrt(1.0 + group_count)[:, None]
    hot_out = hot_sum / jnp.sqrt(1.0 + counts_hot)[:, None]
    return group_out, group_count, hot_out, counts_hot


def solution(mesh):
    in_specs = (P(("owner", "rep"), None), P(("owner", "rep")), P(("owner", "rep")), P(), P())
    out_specs = (P(("owner", "rep"), None), P(("owner", "rep")), P("rep", None), P("rep"))
    return jax.shard_map(local, mesh=mesh, in_specs=in_specs, out_specs=out_specs, check_vma=False)
```

```python
import functools

import jax
import jax.numpy as jnp
from jax import lax
from jax.experimental import pallas as pl
from jax.experimental.pallas import tpu as pltpu
from jax.sharding import PartitionSpec as P

MESH = pl.DeviceIdType.MESH
LANES = 128
SUB = 8
BF = jnp.bfloat16
F32 = jnp.float32


def iota(shape, axis):
    return lax.broadcasted_iota(jnp.int32, shape, axis)


def mm(a, b, dims=((1,), (0,))):
    return lax.dot_general(a, b, (dims, ((), ())), preferred_element_type=F32)


def split(x):
    hi = x.astype(BF)
    return hi, (x - hi.astype(F32)).astype(BF)


def kernel(
    cfg,
    ids_hbm,
    survive_hbm,
    hot_hbm,
    table_hbm,
    feat_hbm,
    sum_ref,
    count_ref,
    hot_sum_ref,
    hot_count_ref,
    ids_ref,
    survive_ref,
    hot_ref,
    table_ref,
    feat_ref,
    bucket,
    arrived,
    tags,
    tags_in,
    hot_part,
    hot_l1,
    hot_s1,
    hot_l2,
    hot_s2,
    hot_l3,
    hot_red,
    hot_all,
    load,
    send1,
    recv1,
    send2,
    recv2,
    tsend,
    trecv,
    s_core,
    r_core,
    s_rep,
    r_rep,
    s_chip,
    r_chip,
    s_all,
    r_all,
    s_last,
    r_last,
):
    owners, reps, cap, own_groups, home_dev = cfg
    rows, width = feat_ref.shape
    hots = hot_ref.shape[1]
    nb = width // cap
    chunks = owners // nb
    chips = owners // 2
    pieces = hots // reps // 2 // SUB
    part = pieces * SUB
    ndev = owners * reps
    half = owners // 2
    quarter = owners // 4
    me = lax.axis_index("owner")
    rep = lax.axis_index("rep")
    dev = me * reps + rep
    core = lax.rem(me, 2)
    chip = me // 2

    loads = [
        pltpu.make_async_copy(src, dst, load.at[i])
        for i, (src, dst) in enumerate(
            (
                (table_hbm, table_ref),
                (ids_hbm, ids_ref),
                (survive_hbm, survive_ref),
                (hot_hbm, hot_ref),
                (feat_hbm, feat_ref),
            )
        )
    ]
    for copy in loads:
        copy.start()

    barrier = pltpu.get_barrier_semaphore()

    @pl.loop(1, ndev)
    def _(d):
        other = lax.rem(dev + d, ndev)
        pl.semaphore_signal(
            barrier, inc=1, device_id=(other // reps, lax.rem(other, reps)), device_id_type=MESH
        )

    flips = []
    bit = 1
    while bit < owners:
        flips.append((bit, bit - 2 * bit * lax.rem(me // bit, 2)))
        bit *= 2

    def partner(p):
        v = p - half
        number = p if p < half else half + v // 2 + (v % 2) * quarter
        out = me
        for bit, flip in flips:
            if number & bit:
                out = out + flip
        return out

    for copy in loads[:4]:
        copy.wait()
    ids = ids_ref[...]
    live_f = jnp.where(survive_ref[...] == 1, 1.0, 0.0)
    table = table_ref[...]
    trows = table.shape[0]
    halves = jnp.concatenate([table >> 8, table & 255], axis=1).astype(F32).astype(BF)
    pick = jnp.where(iota((trows, rows), 0) == (ids >> 7), 1.0, 0.0).astype(BF)
    both = mm(halves, pick, ((0,), (0,)))
    column = both[:LANES] * 256.0 + both[LANES:]
    home = jnp.sum(
        jnp.where(iota((LANES, rows), 0) == (ids & (LANES - 1)), column, 0.0), axis=0, keepdims=True
    )
    target = jnp.floor(home * (1.0 / own_groups))
    label = home - target * own_groups + 1.0
    number = target.astype(jnp.int32) ^ me
    low = number & (half - 1)
    spread = half + 2 * (low & (quarter - 1)) + jnp.where(low >= quarter, 1, 0)
    place_at = jnp.where(number < half, number, spread)

    hot_col = jnp.sum(
        jnp.where(iota((hots, hots), 0) == iota((hots, hots), 1), hot_ref[...].astype(F32), 0.0),
        axis=1,
        keepdims=True,
    )
    matches = jnp.where(hot_col == ids.astype(F32), 1.0, 0.0)
    is_hot = jnp.max(matches, axis=0, keepdims=True)
    keep = live_f * (1.0 - is_hot)
    place_at = jnp.where(keep > 0.0, place_at, -1)

    member = jnp.where(iota((owners, rows), 0) == place_at, 1.0, 0.0)
    before = jnp.where(iota((rows, rows), 0) < iota((rows, rows), 1), 1.0, 0.0).astype(BF)
    position = mm(member.astype(BF), before)
    placed = jnp.sum(position * member, axis=0, keepdims=True).astype(jnp.int32)
    slot = jnp.where(keep > 0.0, place_at * cap + placed, -1)
    lane = placed + cap * (place_at & (nb - 1))
    label_hi = jnp.floor(label * (1.0 / 256.0))
    label_lo = label - 256.0 * label_hi
    coded = jnp.concatenate([member * label_hi, member * label_lo], axis=0).astype(BF)
    where = jnp.where(iota((width, rows), 0) == lane, 1.0, 0.0).astype(BF)
    coded = mm(coded, where, ((1,), (1,)))
    labels = coded[:owners] * 256.0 + coded[owners:]
    for p in range(owners):
        tags[p] = labels[p : p + 1]

    def send_block(p):
        return pltpu.make_async_remote_copy(
            src_ref=bucket.at[p - 1],
            dst_ref=arrived.at[0, p],
            send_sem=send1,
            recv_sem=recv1.at[p],
            device_id=(partner(p), rep),
            device_id_type=MESH,
        )

    def send_tag(q, p):
        return pltpu.make_async_remote_copy(
            src_ref=tags.at[p],
            dst_ref=tags_in.at[q, p],
            send_sem=tsend.at[q, p],
            recv_sem=trecv.at[q, p],
            device_id=(partner(p), lax.rem(rep + q, reps)),
            device_id_type=MESH,
        )

    def forward(q, p):
        return pltpu.make_async_remote_copy(
            src_ref=arrived.at[0, p],
            dst_ref=arrived.at[q, p],
            send_sem=send2,
            recv_sem=recv2.at[q, p],
            device_id=(me, lax.rem(rep + q, reps)),
            device_id_type=MESH,
        )

    pairs = [(q, p) for p in range(owners) for q in range(reps) if q + p]
    tags_in[0, 0] = labels[:1]
    loads[4].wait()
    feat_hi, feat_lo = split(feat_ref[...])
    mate = (me + 1 - 2 * core, rep)
    to_core = pltpu.make_async_remote_copy(
        src_ref=hot_part.at[:, 1 - core],
        dst_ref=hot_l1,
        send_sem=s_core,
        recv_sem=r_core,
        device_id=mate,
        device_id_type=MESH,
    )
    def hot_start():
        hot_table = matches * live_f
        tally = jnp.sum(hot_table, axis=1, keepdims=True)
        hot_bf = hot_table.astype(BF)
        sums = mm(hot_bf, feat_hi) + mm(hot_bf, feat_lo)
        hot_part[:, :, :, :width] = sums.reshape(reps, 2, part, width)
        hot_part[:, :, :, width:] = jnp.broadcast_to(tally, (hots, LANES)).reshape(reps, 2, part, LANES)
        to_core.start()

    for c in range(chunks):
        place = jnp.where(iota((width, rows), 0) + c * width == slot, 1.0, 0.0).astype(BF)
        packed = mm(place, feat_hi) + mm(place, feat_lo)
        for i in range(nb):
            p = c * nb + i
            dst = arrived.at[0, 0] if p == 0 else bucket.at[p - 1]
            dst[...] = packed[i * cap : (i + 1) * cap]
        if c == 0:
            pl.semaphore_wait(barrier, ndev - 1)
        for p in range(c * nb, (c + 1) * nb):
            if p == 0:
                for q in range(1, reps):
                    forward(q, 0).start()
            elif c < chunks - 1:
                send_block(p).start()
        if c == chunks - 2:
            hot_start()
    for q, p in pairs:
        send_tag(q, p).start()

    def to_rep(q):
        other = lax.rem(rep + q, reps)
        return pltpu.make_async_remote_copy(
            src_ref=hot_s1.at[other],
            dst_ref=hot_l2.at[q],
            send_sem=s_rep.at[q],
            recv_sem=r_rep.at[q],
            device_id=(me, other),
            device_id_type=MESH,
        )

    def to_chip(p):
        return pltpu.make_async_remote_copy(
            src_ref=hot_s2.at[p],
            dst_ref=hot_l3.at[lax.rem(p - chip + chips, chips)],
            send_sem=s_chip.at[p],
            recv_sem=r_chip,
            device_id=(p * 2 + core, rep),
            device_id_type=MESH,
        )

    def to_all(d):
        return pltpu.make_async_remote_copy(
            src_ref=hot_red,
            dst_ref=hot_all.at[core, chip],
            send_sem=s_all.at[d],
            recv_sem=r_all.at[chip],
            device_id=(lax.rem(chip + d, chips) * 2 + core, rep),
            device_id_type=MESH,
        )

    to_mate = pltpu.make_async_remote_copy(
        src_ref=hot_all.at[core],
        dst_ref=hot_all.at[core],
        send_sem=s_last,
        recv_sem=r_last,
        device_id=mate,
        device_id_type=MESH,
    )

    def hot_step_1():
        to_core.wait_recv()
        hot_s1[...] = hot_part[:, core] + hot_l1[...]
        for q in range(1, reps):
            to_rep(q).start()

    def hot_step_2():
        total = hot_s1[rep]
        for q in range(1, reps):
            to_rep(q).wait_recv()
            total = total + hot_l2[q]
        hot_s2[...] = total.reshape(pieces, SUB, width + LANES)

        @pl.loop(0, pieces)
        def _(p):
            @pl.when(p != chip)
            def _():
                to_chip(p).start()

    def hot_step_3():
        @pl.when(chip < pieces)
        def _():
            mine = hot_l3.at[pl.ds(1, chips - 1)]
            pltpu.make_async_copy(mine, mine, r_chip).wait()
            total = hot_s2[chip] + jnp.sum(hot_l3[1:], axis=0)
            hot_red[...] = total
            hot_all[core, chip] = total

            @pl.loop(1, chips)
            def _(d):
                to_all(d).start()

    def hot_step_4():
        @pl.loop(0, pieces)
        def _(p):
            @pl.when(p != chip)
            def _():
                pltpu.make_async_copy(hot_all.at[core, p], hot_all.at[core, p], r_all.at[p]).wait()

        to_mate.start()

    def hot_step_5():
        to_mate.wait_recv()
        everything = hot_all[...].reshape(2 * part, width + LANES)
        hot_sum_ref[...] = everything[:, :width]
        counts = everything[:, width:]
        diagonal = jnp.where(iota((2 * part, LANES), 0) == iota((2 * part, LANES), 1), counts, 0.0)
        hot_count_ref[...] = jnp.broadcast_to(jnp.sum(diagonal, axis=0, keepdims=True), (SUB, LANES))

    tiles = max(1, home_dev // 512)
    tile = home_dev // tiles
    base = rep * home_dev + 1

    def add_chunk(q, c):
        first = q == 0 and c == 0
        lab = jnp.zeros((1, width), F32)
        for p in range(c * nb, (c + 1) * nb):
            if q + p:
                send_tag(q, p).wait_recv()
            lab = lab + tags_in[q, p]
        lab = lab.astype(jnp.int32) - base
        block = jnp.concatenate([arrived[q, c * nb + i] for i in range(nb)], axis=0)
        hi, lo = split(block)
        ones = jnp.ones((SUB, width), BF)

        for t in range(tiles):
            onehot = jnp.where(iota((tile, width), 0) + t * tile == lab, 1.0, 0.0).astype(BF)
            at = pl.ds(t * tile, tile)
            total = mm(onehot, hi) + mm(onehot, lo)
            tally = mm(ones, onehot, ((1,), (1,)))
            if first:
                sum_ref[at, :] = total
                count_ref[:, at] = tally
            else:
                sum_ref[at, :] += total
                count_ref[:, at] += tally

    def pass_on(c):
        for p in range(max(1, c * nb), (c + 1) * nb):
            send_block(p).wait_recv()
            for q in range(1, reps):
                forward(q, p).start()

    def peer_chunk(c):
        for q in range(1, reps):
            for p in range(c * nb, (c + 1) * nb):
                forward(q, p).wait_recv()
            add_chunk(q, c)

    hot_step_1()
    pass_on(0)
    add_chunk(0, 0)
    hot_step_2()
    for p in range((chunks - 1) * nb, owners):
        send_block(p).start()
    for c in range(1, chunks - 1):
        pass_on(c)
        if c < chunks - 2:
            add_chunk(0, c)
    hot_step_3()
    pass_on(chunks - 1)
    for c in range(chunks - 2, chunks):
        add_chunk(0, c)
    hot_step_4()
    for c in range(chunks - 1):
        peer_chunk(c)
    hot_step_5()
    peer_chunk(chunks - 1)

    to_core.wait_send()
    for q in range(1, reps):
        to_rep(q).wait_send()

    @pl.loop(0, pieces)
    def _(p):
        @pl.when(p != chip)
        def _():
            to_chip(p).wait_send()

    @pl.when(chip < pieces)
    def _():
        @pl.loop(1, chips)
        def _(d):
            to_all(d).wait_send()

    to_mate.wait_send()
    for q, p in pairs:
        send_tag(q, p).wait_send()
    pltpu.make_async_copy(bucket, bucket, send1).wait()
    if reps > 1:
        sent = arrived.at[pl.ds(1, reps - 1)]
        pltpu.make_async_copy(sent, sent, send2).wait()


def local(features, group_ids, survive, home_row, hot_ids):
    rows, width = features.shape
    owners = lax.axis_size("owner")
    reps = lax.axis_size("rep")
    groups = home_row.shape[0]
    hots = hot_ids.shape[0]
    own_groups = groups // owners
    home_dev = own_groups // reps
    cap = 2 * rows // owners
    chips = owners // 2
    pieces = hots // reps // 2 // SUB
    part = pieces * SUB
    wide = width + LANES
    cfg = (owners, reps, cap, own_groups, home_dev)
    vmem = pl.BlockSpec(memory_space=pltpu.VMEM)
    hbm = pl.BlockSpec(memory_space=pltpu.HBM)
    DMA = pltpu.SemaphoreType.DMA
    VM = pltpu.VMEM
    cold_sum, count, hot_sum, hot_count = pl.pallas_call(
        functools.partial(kernel, cfg),
        out_shape=(
            jax.ShapeDtypeStruct((home_dev, width), F32),
            jax.ShapeDtypeStruct((SUB, home_dev), F32),
            jax.ShapeDtypeStruct((hots // reps, width), F32),
            jax.ShapeDtypeStruct((SUB, LANES), F32),
        ),
        in_specs=[hbm] * 5,
        out_specs=[vmem] * 4,
        scratch_shapes=[
            VM((1, rows), jnp.int32),
            VM((1, rows), jnp.int32),
            VM((1, hots), jnp.int32),
            VM((groups // LANES, LANES), jnp.int32),
            VM((rows, width), F32),
            VM((owners - 1, cap, width), F32),
            VM((reps, owners, cap, width), F32),
            VM((owners, 1, width), F32),
            VM((reps, owners, 1, width), F32),
            VM((reps, 2, part, wide), F32),
            VM((reps, part, wide), F32),
            VM((reps, part, wide), F32),
            VM((reps, part, wide), F32),
            VM((pieces, SUB, wide), F32),
            VM((chips, SUB, wide), F32),
            VM((SUB, wide), F32),
            VM((2, pieces, SUB, wide), F32),
            DMA((5,)),
            DMA(()),
            DMA((owners,)),
            DMA(()),
            DMA((reps, owners)),
            DMA((reps, owners)),
            DMA((reps, owners)),
            DMA(()),
            DMA(()),
            DMA((reps,)),
            DMA((reps,)),
            DMA((pieces,)),
            DMA(()),
            DMA((chips,)),
            DMA((pieces,)),
            DMA(()),
            DMA(()),
        ],
        compiler_params=pltpu.CompilerParams(
            collective_id=0, has_side_effects=True, vmem_limit_bytes=48 << 20
        ),
    )(
        group_ids.reshape(1, rows),
        survive.reshape(1, rows),
        hot_ids.reshape(1, hots),
        home_row.reshape(groups // LANES, LANES),
        features,
    )
    group_count = count[0]
    counts_hot = hot_count[0, : hots // reps]
    group_out = cold_sum / jnp.sqrt(1.0 + group_count)[:, None]
    hot_out = hot_sum / jnp.sqrt(1.0 + counts_hot)[:, None]
    return group_out, group_count, hot_out, counts_hot


def solution(mesh):
    in_specs = (P(("owner", "rep"), None), P(("owner", "rep")), P(("owner", "rep")), P(), P())
    out_specs = (P(("owner", "rep"), None), P(("owner", "rep")), P("rep", None), P("rep"))
    return jax.shard_map(local, mesh=mesh, in_specs=in_specs, out_specs=out_specs, check_vma=False)
```
